32 devices in a mesh: cells: 8 (over z, y), grp: 4 (over x, core).
Axes of the slice: x: 2, y: 2, z: 4, core: 2. Of those that a mesh axis runs over, the one named last changes fastest.
Arguments:
- latent_coordinates: float32 [50, 131072], P(None, ('cells', 'grp')), may hold values from -40 to 40
- group_means: float32 [16, 50], replicated, may hold values from -4 to 4
- entropy_scaling: float32 [16], replicated, may hold values from 0.5 to 2
- sample_shrinkage_lambda: float32 [200], replicated, may hold values from 164 to 1310
- sample_population: int32 [200], replicated, may hold values from 1 to 1310, 131072 in all
Outputs:
- corrected: float32 [50, 131072], P(None, ('cells', 'grp'))
- new_centroids: float32 [16, 50], P('cells')
The draws below stay inside these ranges and needn't reach their ends.
All inputs are finite; a program needn't handle non-finite values.
Results may differ from the reference program's by a relative error of at most 0.0003.
Values sent between devices are 32-bit elements; how exact they have to be, the bound alone decides.
A program may use at most 64 MiB of HBM per device.

```python
import math
import jax
import jax.numpy as jnp
import numpy as np
from jax import lax

PCS = 50
GROUP_NUMBER = 16
NB = 200
CELLS = 131072
MOST = 1310


def centre_table(key):
    table = jax.random.normal(jax.random.fold_in(key, 11), (GROUP_NUMBER, PCS), jnp.float32) * 0.5
    return table


def draw_group_means(key, part):
    return jnp.clip(centre_table(key), -4.0, 4.0)


def draw_latent_coordinates(key, part):
    region_len = CELLS // NB
    shifts = jax.random.normal(jax.random.fold_in(key, 2), (PCS, NB + 1), jnp.float32)
    region = jnp.minimum(jnp.arange(CELLS) // region_len, NB)
    offset = shifts[:, region]
    noise = jax.random.normal(jax.random.fold_in(key, 1), (PCS, CELLS), jnp.float32)
    values = noise + offset
    return jnp.clip(values, -40.0, 40.0)


def split_up(count, total, most, skew):
    portions = [(1 << 20) // math.isqrt(rank ** skew) + 1 for rank in range(2, count + 1)]
    rest, given = total - most - (count - 1), [1] * (count - 1)
    while rest > 0:
        movable = [i for i in range(count - 1) if given[i] < most]
        whole, remaining = sum([portions[i] for i in movable]), rest
        for i in movable:
            more = min(most - given[i], max(1, remaining * portions[i] // whole), rest)
            given[i] = given[i] + more
            rest = rest - more
    return np.array([most] + given)


def ragged(rng, count, total, limit, lean):
    if count == 2:
        one = jax.random.randint(rng, (), max(1, total - limit), min(limit, total - 1) + 1)
        return jnp.stack([one, total - one])
    tallies = jnp.asarray(split_up(count, total, limit, lean), jnp.int32)
    twos = (count - 1) // 2
    giver, receiver = tallies[1:1 + 2 * twos:2], tallies[2:2 + 2 * twos:2]
    slack = jnp.minimum(giver - 1, limit - receiver)
    shifted = jax.random.randint(jax.random.fold_in(rng, 1), (twos,), 0, 1 << 20) % (slack + 1)
    tallies = tallies.at[1:1 + 2 * twos:2].set(giver - shifted).at[2:2 + 2 * twos:2].set(receiver + shifted)
    return tallies[jax.random.permutation(jax.random.fold_in(rng, 2), count)]


def setup_inputs(seed: int = 0) -> dict:
    key_list = jax.random.split(jax.random.key(seed), 6)
    latent_coordinates = draw_latent_coordinates(jax.random.fold_in(key_list[5], 71), 0)
    group_means = draw_group_means(jax.random.fold_in(key_list[5], 71), 0)
    entropy_scaling = jnp.clip(jnp.exp(jax.random.uniform(key_list[2], (GROUP_NUMBER,), jnp.float32, math.log(0.5), math.log(2.0))), 0.5, 2.0)
    sample_shrinkage_lambda = jnp.clip(jnp.exp(jax.random.uniform(key_list[3], (NB,), jnp.float32, math.log(164.0), math.log(1310.0))), 164.0, 1310.0)
    sample_population = ragged(key_list[4], NB, CELLS, MOST, 2).astype(jnp.int32)
    return {"latent_coordinates": latent_coordinates, "group_means": group_means, "entropy_scaling": entropy_scaling, "sample_shrinkage_lambda": sample_shrinkage_lambda, "sample_population": sample_population}


diversity = 2.0
intercept_ridge = 1.0
highest = lax.Precision.HIGHEST


def observation_affinity(latent_coordinates, group_means, entropy_scaling):
    pairwise_dots = jnp.dot(group_means, latent_coordinates, precision=highest, preferred_element_type=jnp.float32)
    quadratic_lengths = jnp.sum(group_means * group_means, axis=1)
    return (2.0 * pairwise_dots - quadratic_lengths[:, None]) / (2.0 * entropy_scaling[:, None])


def probabilistic_responsibility(group_affinity):
    top = jnp.max(group_affinity, axis=0, keepdims=True)
    raised = jnp.exp(group_affinity - top)
    return raised / jnp.sum(raised, axis=0, keepdims=True)


def reference(latent_coordinates, group_means, entropy_scaling, sample_shrinkage_lambda, sample_population):
    cells_total = latent_coordinates.shape[1]
    batch_ends = jnp.cumsum(sample_population).astype(jnp.int32)
    batch_starts = (batch_ends - sample_population).astype(jnp.int32)
    padded = jnp.pad(latent_coordinates, ((0, 0), (0, MOST)))
    window = lax.iota(jnp.int32, MOST)

    def batch_cells(start, size):
        contiguous_portion = lax.dynamic_slice(padded, (jnp.int32(0), start), (PCS, MOST))
        inside = (window < size).astype(jnp.float32)
        return contiguous_portion, inside

    def count_step(carry, item):
        start, size = item
        contiguous_portion, inside = batch_cells(start, size)
        expected_occupancy = probabilistic_responsibility(observation_affinity(contiguous_portion, group_means, entropy_scaling))
        return carry, jnp.sum(expected_occupancy * inside[None, :], axis=1)

    unused, counts_t = lax.scan(count_step, jnp.float32(0.0), (batch_starts, sample_population))
    counts = counts_t.T
    totals = jnp.sum(counts, axis=1)
    expected = sample_population.astype(jnp.float32)[None, :] * totals[:, None] / jnp.float32(cells_total)
    penalty = diversity * jnp.log((counts + 1.0) / (expected + 1.0))

    def assign_of(contiguous_portion, single_observation):
        return probabilistic_responsibility(observation_affinity(contiguous_portion, group_means, entropy_scaling) - single_observation[:, None])

    def moment_step(carry, item):
        start, size, single_observation = item
        contiguous_portion, inside = batch_cells(start, size)
        assign = assign_of(contiguous_portion, single_observation) * inside[None, :]
        augmented = jnp.concatenate([jnp.ones((1, MOST), jnp.float32), contiguous_portion], axis=0)
        return carry, jnp.einsum("kn,dn->kd", assign, augmented, precision=highest)

    unused, moments_t = lax.scan(moment_step, jnp.float32(0.0), (batch_starts, sample_population, penalty.T))
    moments = jnp.transpose(moments_t, (1, 2, 0))
    mass = moments[:, 0, :]
    sums = moments[:, 1:, :]
    shrink = sample_shrinkage_lambda[None, :] / (mass + sample_shrinkage_lambda[None, :])
    weight = jnp.sum(mass * shrink, axis=1)
    right_side = jnp.sum(sums * shrink[:, None, :], axis=2)
    intercept = right_side / (intercept_ridge + weight)[:, None]
    coefficients = (sums - mass[:, None, :] * intercept[:, :, None]) / (mass + sample_shrinkage_lambda[None, :])[:, None, :]
    new_centroids = jnp.sum(sums, axis=2) / (1.0 + jnp.sum(mass, axis=1))[:, None]

    def correct_step(carry, item):
        start, size, single_observation, coef = item
        contiguous_portion, inside = batch_cells(start, size)
        assign = assign_of(contiguous_portion, single_observation) * inside[None, :]
        moved = jnp.einsum("kd,kn->dn", coef, assign, precision=highest)
        current = lax.dynamic_slice(carry, (jnp.int32(0), start), (PCS, MOST))
        fresh = jnp.where(inside[None, :] > 0.0, contiguous_portion - moved, current)
        return lax.dynamic_update_slice(carry, fresh, (jnp.int32(0), start)), jnp.float32(0.0)

    result, unused = lax.scan(correct_step, padded, (batch_starts, sample_population, penalty.T, jnp.transpose(coefficients, (2, 0, 1))))
    return result[:, :cells_total], new_centroids
```

```python
import functools

import jax
import jax.numpy as jnp
from jax import lax
from jax.experimental import pallas as pl
from jax.experimental.pallas import tpu as pltpu
from jax.sharding import PartitionSpec as P

diversity = 2.0
intercept_ridge = 1.0
highest = lax.Precision.HIGHEST


def from_behind(block, axis, distance):
    devices = range(lax.axis_size(axis))
    route = [(i - distance, i) for i in devices if i - distance in devices]
    return lax.ppermute(block, axis, route)


def observation_affinity(latent_coordinates, group_means, entropy_scaling):
    pairwise_dots = jnp.dot(
        group_means, latent_coordinates, precision=highest, preferred_element_type=jnp.float32
    )
    quadratic_lengths = jnp.sum(group_means * group_means, axis=1)
    return (2.0 * pairwise_dots - quadratic_lengths[:, None]) / (2.0 * entropy_scaling[:, None])


def probabilistic_responsibility(group_affinity):
    top = jnp.max(group_affinity, axis=0, keepdims=True)
    raised = jnp.exp(group_affinity - top)
    return raised / jnp.sum(raised, axis=0, keepdims=True)


def batch_parts(moments, ridge):
    mass = moments[:, 0, :]
    sums = moments[:, 1:, :]
    shrink = ridge[None, :] / (mass + ridge[None, :])
    weight = jnp.sum(mass * shrink, axis=1)
    right_side = jnp.sum(sums * shrink[:, None, :], axis=2)
    return (weight, right_side, jnp.sum(mass, axis=1), jnp.sum(sums, axis=2))


def slopes_of(moments, ridge, weight, right_side):
    mass = moments[:, 0, :]
    sums = moments[:, 1:, :]
    intercept = right_side / (intercept_ridge + weight)[:, None]
    return (sums - mass[:, None, :] * intercept[:, :, None]) / (mass + ridge[None, :])[:, None, :]


def body(
    latent_coordinates, group_means, entropy_scaling, sample_shrinkage_lambda, sample_population
):
    local_cells = latent_coordinates.shape[1]
    num_pcs = latent_coordinates.shape[0]
    clusters = group_means.shape[0]
    batches = sample_population.shape[0]
    owned = clusters // lax.axis_size("cells")
    offset = (lax.axis_index("cells") * lax.axis_size("grp") + lax.axis_index("grp")) * local_cells
    batch_ends = jnp.cumsum(sample_population)
    batch_starts = batch_ends - sample_population
    cells_total = jnp.sum(sample_population).astype(jnp.float32)
    position = offset + lax.iota(jnp.int32, local_cells)
    batch_of = jnp.sum((batch_ends[:, None] <= position[None, :]).astype(jnp.int32), axis=0)
    first_batch = batch_of[0]
    last_batch = batch_of[local_cells - 1]
    group_affinity = observation_affinity(latent_coordinates, group_means, entropy_scaling)
    expected_occupancy = probabilistic_responsibility(group_affinity)

    def count_step(batch_id, running):
        in_batch = (batch_of == batch_id).astype(jnp.float32)
        single_observation = jnp.dot(
            expected_occupancy, in_batch, precision=highest, preferred_element_type=jnp.float32
        )
        return lax.dynamic_update_slice(
            running, single_observation[:, None], (jnp.int32(0), batch_id)
        )

    counts = lax.fori_loop(
        first_batch, last_batch + 1, count_step, jnp.zeros((clusters, batches), jnp.float32)
    )
    counts = lax.psum(counts, ("cells", "grp"))
    totals = jnp.sum(counts, axis=1)
    expected = sample_population.astype(jnp.float32)[None, :] * totals[:, None] / cells_total
    penalty = diversity * jnp.log((counts + 1.0) / (expected + 1.0))

    def penalty_step(batch_id, running):
        in_batch = (batch_of == batch_id).astype(jnp.float32)
        column = lax.dynamic_index_in_dim(penalty, batch_id, 1, keepdims=True)
        return running + column * in_batch[None, :]

    cell_penalty = lax.fori_loop(
        first_batch, last_batch + 1, penalty_step, jnp.zeros((clusters, local_cells), jnp.float32)
    )
    assign = probabilistic_responsibility(group_affinity - cell_penalty)
    augmented = jnp.concatenate(
        [jnp.ones((1, local_cells), jnp.float32), latent_coordinates], axis=0
    )

    def moment_step(batch_id, running):
        in_batch = (batch_of == batch_id).astype(jnp.float32)
        contiguous_portion = jnp.einsum(
            "kn,dn->kd", assign * in_batch[None, :], augmented, precision=highest
        )
        return lax.dynamic_update_slice(
            running, contiguous_portion[:, :, None], (jnp.int32(0), jnp.int32(0), batch_id)
        )

    moments = lax.fori_loop(
        first_batch,
        last_batch + 1,
        moment_step,
        jnp.zeros((clusters, num_pcs + 1, batches), jnp.float32),
    )
    devices_flat = lax.axis_size("cells") * lax.axis_size("grp")
    most_cells = 2 * local_cells * devices_flat // batches
    reach = (most_cells - 2) // local_cells + 1
    begins_here = (batch_starts >= offset) & (batch_starts < offset + local_cells)
    owner_mask = begins_here.astype(jnp.float32)
    head_owned = begins_here[first_batch]
    head_column = lax.dynamic_index_in_dim(moments, first_batch, 2, keepdims=False)
    sent_stats = jnp.where(head_owned, 0.0, 1.0) * head_column
    sent_tag = jnp.where(head_owned, 0.0, first_batch.astype(jnp.float32) + 1.0) * jnp.ones(
        (1,), jnp.float32
    )
    completed = moments
    for hop in range(1, reach + 1):
        got_stats, got_tag = from_behind((sent_stats, sent_tag), ("cells", "grp"), -hop)
        got_id = jnp.maximum(got_tag[0].astype(jnp.int32) - 1, 0)
        accept = jnp.where((got_tag[0] > 0.5) & begins_here[got_id], 1.0, 0.0)
        single_observation = (
            lax.dynamic_index_in_dim(completed, got_id, 2, keepdims=False) + accept * got_stats
        )
        completed = lax.dynamic_update_slice(
            completed, single_observation[:, :, None], (jnp.int32(0), jnp.int32(0), got_id)
        )
    completed = completed * owner_mask[None, None, :]
    weight, right_side, mass_total, moment_total = lax.psum(
        batch_parts(completed, sample_shrinkage_lambda), ("cells", "grp")
    )
    coefficients = slopes_of(completed, sample_shrinkage_lambda, weight, right_side)
    every_centroid = moment_total / (1.0 + mass_total)[:, None]
    new_centroids = lax.dynamic_slice_in_dim(
        every_centroid, lax.axis_index("cells") * owned, owned, 0
    )
    tail_owned = begins_here[last_batch]
    tail_column = lax.dynamic_index_in_dim(coefficients, last_batch, 2, keepdims=False)
    tail_send = jnp.where(tail_owned, 1.0, 0.0) * tail_column
    tail_tag = jnp.where(tail_owned, last_batch.astype(jnp.float32) + 1.0, 0.0) * jnp.ones(
        (1,), jnp.float32
    )
    head_fix = jnp.zeros_like(tail_column)
    for hop in range(1, reach + 1):
        got_coef, got_tag = from_behind((tail_send, tail_tag), ("cells", "grp"), hop)
        match = got_tag[0] == first_batch.astype(jnp.float32) + 1.0
        head_fix = jnp.where(match, got_coef, head_fix)
    own_head = lax.dynamic_index_in_dim(coefficients, first_batch, 2, keepdims=False)
    head_final = jnp.where(head_owned, own_head, head_fix)
    coefficients = lax.dynamic_update_slice(
        coefficients, head_final[:, :, None], (jnp.int32(0), jnp.int32(0), first_batch)
    )

    def correct_step(batch_id, running):
        in_batch = (batch_of == batch_id).astype(jnp.float32)
        slope_table = lax.dynamic_index_in_dim(coefficients, batch_id, 2, keepdims=False)
        moved = jnp.einsum("kd,kn->dn", slope_table, assign * in_batch[None, :], precision=highest)
        return running - moved

    corrected = lax.fori_loop(first_batch, last_batch + 1, correct_step, latent_coordinates)
    return (corrected, new_centroids)


SLOTS = 16
MESH = pl.DeviceIdType.MESH
f32 = jnp.float32
bf16 = jnp.bfloat16


def hi_lo(value):
    hi = value.astype(bf16)
    return hi, (value - hi.astype(f32)).astype(bf16)


def nt_dot(a, b):
    return lax.dot_general(a, b, (((1,), (1,)), ((), ())), preferred_element_type=f32)


def nn_dot(a, b):
    return jnp.dot(a, b, preferred_element_type=f32)


def iota(shape, axis):
    return lax.broadcasted_iota(jnp.int32, shape, axis)


def fiota(shape, axis):
    return iota(shape, axis).astype(f32)


def fused_kernel(
    cells_size, grp_size, chunk,
    x_ref, means_ref, entropy_ref, ridge_ref, population_ref,
    out_ref, centroid_ref,
    xs, xcat, scores, mask, zh, zl, send1, recv1, send_a, recv_a, slab1, slab2,
    sem1, sem_a, sem_b, sem_c,
):
    num_pcs, local = x_ref.shape
    clusters = means_ref.shape[0]
    batches = population_ref.shape[1]
    owned = centroid_ref.shape[0]
    rows = SLOTS * clusters
    wide = xs.shape[0]
    devices = cells_size * grp_size
    chunks = local // chunk
    cell_index = lax.axis_index("cells")
    grp_index = lax.axis_index("grp")
    me = cell_index * grp_size + grp_index

    def at(flat):
        return {"cells": flat // grp_size, "grp": lax.rem(flat, grp_size)}

    barrier = pltpu.get_barrier_semaphore()
    for step in range(1, devices):
        pl.semaphore_signal(
            barrier, inc=1, device_id=at(lax.rem(me + step, devices)), device_id_type=MESH
        )

    population = population_ref[...].astype(f32)
    ridge = ridge_ref[...]
    offset = (me * local).astype(f32)
    ends = jnp.sum(
        jnp.where(iota((batches, batches), 1) <= iota((batches, batches), 0), population, 0.0),
        axis=1, keepdims=True,
    )

    def batch_at(position):
        return jnp.sum(jnp.where(ends <= position, 1.0, 0.0), axis=0, keepdims=True)

    first = batch_at(offset)
    last = batch_at(offset + (local - 1.0))
    prev_last = batch_at(offset - 1.0)
    next_first = batch_at(offset + float(local))
    tail_slot = last - first
    from_prev = jnp.where((prev_last == first) & (first * 0.0 + offset > 0.0), 1.0, 0.0)
    from_next = jnp.where(next_first == last, 1.0, 0.0)
    lane = fiota((SLOTS, batches), 1)
    slot = first + fiota((SLOTS, 1), 0)
    slot_start = jnp.sum(jnp.where(lane < slot, population, 0.0), axis=1, keepdims=True)
    slot_size = jnp.sum(jnp.where(lane == slot, population, 0.0), axis=1, keepdims=True)
    slot_end = slot_start + slot_size
    cells_total = jnp.sum(population, axis=1, keepdims=True)
    size_row = jnp.sum(
        jnp.where(iota((SLOTS, SLOTS), 0) == iota((SLOTS, SLOTS), 1), slot_size, 0.0),
        axis=0, keepdims=True,
    )
    row_slot = first + (iota((rows, 1), 0) // clusters).astype(f32)
    row_ridge = jnp.sum(
        jnp.where(fiota((rows, batches), 1) == row_slot, ridge, 0.0), axis=1, keepdims=True
    )
    row_ridge = jnp.where(row_slot < float(batches), row_ridge, 1.0)

    means = means_ref[...]
    lengths = jnp.sum(means * means, axis=1, keepdims=True)
    twice = 2.0 * entropy_ref[...]

    xs[num_pcs - num_pcs % 8 :, :] = jnp.where(
        iota((wide - num_pcs + num_pcs % 8, local), 0) == num_pcs % 8, 1.0, 0.0
    )
    xs[:num_pcs, :] = x_ref[...]

    def scores_step(index, counts):
        at_lanes = pl.ds(pl.multiple_of(index * chunk, chunk), chunk)
        block = xs[:, at_lanes]
        hi, lo = hi_lo(block)
        xcat[:wide, at_lanes] = hi
        xcat[wide:, at_lanes] = lo
        dots = jnp.dot(
            means, block[:num_pcs], precision=highest, preferred_element_type=f32
        )
        affinity = (2.0 * dots - lengths) / twice
        scores[:, at_lanes] = affinity
        prior = probabilistic_responsibility(affinity)
        position = offset + (index * chunk).astype(f32) + fiota((1, chunk), 1)
        inside = jnp.where(
            (position >= slot_start) & (position < slot_end), 1.0, 0.0
        ).astype(bf16)
        mask[:, at_lanes] = inside
        prior_hi, prior_lo = hi_lo(prior)
        return counts + nt_dot(prior_hi, inside) + nt_dot(prior_lo, inside)

    counts = lax.fori_loop(0, chunks, scores_step, jnp.zeros((clusters, SLOTS), f32))

    slot_lane = fiota((clusters, SLOTS), 1)
    total = jnp.sum(counts, axis=1, keepdims=True)
    tail = jnp.sum(jnp.where(slot_lane == tail_slot, counts, 0.0), axis=1, keepdims=True)
    width = send1.shape[2]
    row_lane = iota((clusters, width), 1)
    row_k = iota((clusters, width), 0)
    packed = (
        jnp.where(row_lane == row_k, total, 0.0)
        + jnp.where(row_lane == row_k + clusters, counts[:, :1], 0.0)
        + jnp.where(row_lane == row_k + 2 * clusters, tail, 0.0)
    )
    packed = jnp.sum(packed, axis=0, keepdims=True)
    send1[0] = packed
    pl.semaphore_wait(barrier, devices - 1)
    for step in range(1, devices):
        pltpu.make_async_remote_copy(
            src_ref=send1.at[0], dst_ref=recv1.at[step - 1],
            send_sem=sem1.at[0], recv_sem=sem1.at[1],
            device_id=at(lax.rem(me + step, devices)), device_id_type=MESH,
        ).start()
    pltpu.make_async_copy(recv1, recv1, sem1.at[1]).wait()

    def column(row, part):
        return jnp.sum(
            jnp.where(row_lane == row_k + part * clusters, row, 0.0), axis=1, keepdims=True
        )

    everyone = packed
    for step in range(1, devices):
        everyone = everyone + recv1[step - 1]
    totals = column(everyone, 0)
    head_more = from_prev * column(recv1[0], 2)
    tail_more = from_next * column(recv1[devices - 2], 1)
    counts = (
        counts
        + jnp.where(slot_lane == 0.0, head_more, 0.0)
        + jnp.where(slot_lane == tail_slot, tail_more, 0.0)
    )
    expected = size_row * totals / cells_total
    penalty = diversity * jnp.log((counts + 1.0) / (expected + 1.0))
    pen_hi = penalty.astype(bf16)
    rest = penalty - pen_hi.astype(f32)
    pen_mid, pen_lo = hi_lo(rest)
    pen_cat = jnp.concatenate([pen_hi, pen_mid, pen_lo], axis=0)

    def assign_step(index, moments):
        at_lanes = pl.ds(pl.multiple_of(index * chunk, chunk), chunk)
        inside = mask[:, at_lanes]
        cell_penalty = nn_dot(pen_cat, inside)
        cell_penalty = (
            cell_penalty[:clusters]
            + cell_penalty[clusters : 2 * clusters]
            + cell_penalty[2 * clusters :]
        )
        assign = probabilistic_responsibility(scores[:, at_lanes] - cell_penalty)
        hi, lo = hi_lo(assign)
        for j in range(SLOTS):
            here = inside[j : j + 1, :]
            zh[j * clusters : (j + 1) * clusters, at_lanes] = hi * here
            zl[j * clusters : (j + 1) * clusters, at_lanes] = lo * here
        first_part = nt_dot(zh[:, at_lanes], xcat[:, at_lanes])
        second_part = nt_dot(zl[:, at_lanes], xcat[:wide, at_lanes])
        return moments + first_part[:, :wide] + first_part[:, wide:] + second_part

    moments = lax.fori_loop(0, chunks, assign_step, jnp.zeros((rows, wide), f32))

    def of_slot(array, j):
        return array[j * clusters : (j + 1) * clusters]

    tail_block = jnp.zeros((clusters, wide), f32)
    for j in range(SLOTS):
        tail_block = tail_block + jnp.where(tail_slot == float(j), of_slot(moments, j), 0.0)
    send_a[0] = tail_block
    send_a[1] = of_slot(moments, 0)
    to_next = pltpu.make_async_remote_copy(
        src_ref=send_a.at[0], dst_ref=recv_a.at[0], send_sem=sem_a.at[0], recv_sem=sem_a.at[1],
        device_id=at(lax.rem(me + 1, devices)), device_id_type=MESH,
    )
    to_prev = pltpu.make_async_remote_copy(
        src_ref=send_a.at[1], dst_ref=recv_a.at[1], send_sem=sem_a.at[2], recv_sem=sem_a.at[3],
        device_id=at(lax.rem(me + devices - 1, devices)), device_id_type=MESH,
    )
    to_next.start()
    to_prev.start()
    to_next.wait_recv()
    to_prev.wait_recv()
    head_more = from_prev * recv_a[0]
    tail_more = from_next * recv_a[1]
    full = []
    for j in range(SLOTS):
        block = of_slot(moments, j) + jnp.where(tail_slot == float(j), tail_more, 0.0)
        full.append(block + head_more if j == 0 else block)

    shrunk_sum = jnp.zeros((clusters, wide), f32)
    plain_sum = jnp.zeros((clusters, wide), f32)
    for j in range(SLOTS):
        lam = of_slot(row_ridge, j)
        shrink = lam / (full[j][:, num_pcs : num_pcs + 1] + lam)
        shrunk_sum = shrunk_sum + shrink * of_slot(moments, j)
        plain_sum = plain_sum + of_slot(moments, j)

    def exchange(slab, value, axis, index, size, sem):
        slab[index] = value
        copies = []
        for step in range(1, size):
            copies.append(
                pltpu.make_async_remote_copy(
                    src_ref=slab.at[index], dst_ref=slab.at[index],
                    send_sem=sem.at[0, step], recv_sem=sem.at[1, step],
                    device_id={axis: lax.rem(index + step, size)}, device_id_type=MESH,
                )
            )
        for copy in copies:
            copy.start()
        for copy in copies:
            copy.wait_recv()
        result = slab[0]
        for step in range(1, size):
            result = result + slab[step]
        return result, copies

    part = jnp.concatenate([shrunk_sum, plain_sum], axis=1)
    part, copies_b = exchange(slab1, part, "grp", grp_index, grp_size, sem_b)
    part, copies_c = exchange(slab2, part, "cells", cell_index, cells_size, sem_c)

    shrunk_sum, plain_sum = part[:, :wide], part[:, wide:]
    intercept = shrunk_sum / (intercept_ridge + shrunk_sum[:, num_pcs : num_pcs + 1])
    centroids = plain_sum / (1.0 + plain_sum[:, num_pcs : num_pcs + 1])
    for r in range(owned):
        picked = jnp.where(
            iota((clusters, wide), 0) == cell_index * owned + r, centroids, 0.0
        )
        centroid_ref[r : r + 1, :] = jnp.sum(picked, axis=0, keepdims=True)[:, :num_pcs]

    slopes = []
    for j in range(SLOTS):
        mass = full[j][:, num_pcs : num_pcs + 1]
        slopes.append((full[j] - mass * intercept) / (mass + of_slot(row_ridge, j)))
    slopes = jnp.concatenate(slopes, axis=0).T
    slope_hi, slope_lo = hi_lo(slopes)
    slope_cat = jnp.concatenate([slope_hi, slope_lo], axis=0)

    def correct_step(index, unused):
        at_lanes = pl.ds(pl.multiple_of(index * chunk, chunk), chunk)
        first_part = nn_dot(slope_cat, zh[:, at_lanes])
        second_part = nn_dot(slope_hi, zl[:, at_lanes])
        moved = first_part[:wide] + first_part[wide:] + second_part
        out_ref[:, at_lanes] = (xs[:, at_lanes] - moved)[:num_pcs]
        return unused

    lax.fori_loop(0, chunks, correct_step, 0)

    pltpu.make_async_copy(recv1, recv1, sem1.at[0]).wait()
    to_next.wait_send()
    to_prev.wait_send()
    for copy in copies_b + copies_c:
        copy.wait_send()


def fused(latent_coordinates, group_means, entropy_scaling, ridge, population):
    num_pcs, local = latent_coordinates.shape
    clusters = group_means.shape[0]
    cells_size, grp_size = lax.axis_size("cells"), lax.axis_size("grp")
    devices = cells_size * grp_size
    rows = SLOTS * clusters
    wide = -(-(num_pcs + 1) // 64) * 64
    width = -(-3 * clusters // 128) * 128
    vmem = pl.BlockSpec(memory_space=pltpu.VMEM)
    dma = pltpu.SemaphoreType.DMA
    return pl.pallas_call(
        functools.partial(fused_kernel, cells_size, grp_size, min(local, 512)),
        out_shape=(
            jax.ShapeDtypeStruct((num_pcs, local), f32),
            jax.ShapeDtypeStruct((clusters // cells_size, num_pcs), f32),
        ),
        in_specs=[vmem] * 5,
        out_specs=(vmem, vmem),
        scratch_shapes=[
            pltpu.VMEM((wide, local), f32),
            pltpu.VMEM((2 * wide, local), bf16),
            pltpu.VMEM((clusters, local), f32),
            pltpu.VMEM((SLOTS, local), bf16),
            pltpu.VMEM((rows, local), bf16),
            pltpu.VMEM((rows, local), bf16),
            pltpu.VMEM((1, 1, width), f32),
            pltpu.VMEM((devices - 1, 1, width), f32),
            pltpu.VMEM((2, clusters, wide), f32),
            pltpu.VMEM((2, clusters, wide), f32),
            pltpu.VMEM((grp_size, clusters, 2 * wide), f32),
            pltpu.VMEM((cells_size, clusters, 2 * wide), f32),
            dma((2,)),
            dma((4,)),
            dma((2, grp_size)),
            dma((2, cells_size)),
        ],
        compiler_params=pltpu.CompilerParams(
            collective_id=0, has_side_effects=True, vmem_limit_bytes=40 * 2**20
        ),
    )(
        latent_coordinates, group_means, entropy_scaling[:, None], ridge[None, :],
        population[None, :],
    )


def step(
    latent_coordinates, group_means, entropy_scaling, sample_shrinkage_lambda, sample_population
):
    local = latent_coordinates.shape[1]
    batches = sample_population.shape[0]
    devices = lax.axis_size("cells") * lax.axis_size("grp")
    args = (
        latent_coordinates, group_means, entropy_scaling, sample_shrinkage_lambda,
        sample_population,
    )
    if 2 * local * devices // batches > local:
        return body(*args)
    ends = jnp.cumsum(sample_population)
    crowded = jnp.any(
        ends[SLOTS - 1 : batches - 1] // local == (ends[: batches - SLOTS] - 1) // local
    )
    return lax.cond(crowded, body, fused, *args)


def solution(mesh):
    return jax.shard_map(
        step,
        mesh=mesh,
        in_specs=(P(None, ("cells", "grp")), P(), P(), P(), P()),
        out_specs=(P(None, ("cells", "grp")), P("cells", None)),
        check_vma=False,
    )
```

```python
import functools

import jax
import jax.numpy as jnp
from jax import lax
from jax.experimental import pallas as pl
from jax.experimental.pallas import tpu as pltpu
from jax.sharding import PartitionSpec as P

diversity = 2.0
intercept_ridge = 1.0
highest = lax.Precision.HIGHEST


def from_behind(block, axis, distance):
    devices = range(lax.axis_size(axis))
    route = [(i - distance, i) for i in devices if i - distance in devices]
    return lax.ppermute(block, axis, route)


def observation_affinity(latent_coordinates, group_means, entropy_scaling):
    pairwise_dots = jnp.dot(
        group_means, latent_coordinates, precision=highest, preferred_element_type=jnp.float32
    )
    quadratic_lengths = jnp.sum(group_means * group_means, axis=1)
    return (2.0 * pairwise_dots - quadratic_lengths[:, None]) / (2.0 * entropy_scaling[:, None])


def probabilistic_responsibility(group_affinity):
    top = jnp.max(group_affinity, axis=0, keepdims=True)
    raised = jnp.exp(group_affinity - top)
    return raised / jnp.sum(raised, axis=0, keepdims=True)


def batch_parts(moments, ridge):
    mass = moments[:, 0, :]
    sums = moments[:, 1:, :]
    shrink = ridge[None, :] / (mass + ridge[None, :])
    weight = jnp.sum(mass * shrink, axis=1)
    right_side = jnp.sum(sums * shrink[:, None, :], axis=2)
    return (weight, right_side, jnp.sum(mass, axis=1), jnp.sum(sums, axis=2))


def slopes_of(moments, ridge, weight, right_side):
    mass = moments[:, 0, :]
    sums = moments[:, 1:, :]
    intercept = right_side / (intercept_ridge + weight)[:, None]
    return (sums - mass[:, None, :] * intercept[:, :, None]) / (mass + ridge[None, :])[:, None, :]


def body(
    latent_coordinates, group_means, entropy_scaling, sample_shrinkage_lambda, sample_population
):
    local_cells = latent_coordinates.shape[1]
    num_pcs = latent_coordinates.shape[0]
    clusters = group_means.shape[0]
    batches = sample_population.shape[0]
    owned = clusters // lax.axis_size("cells")
    offset = (lax.axis_index("cells") * lax.axis_size("grp") + lax.axis_index("grp")) * local_cells
    batch_ends = jnp.cumsum(sample_population)
    batch_starts = batch_ends - sample_population
    cells_total = jnp.sum(sample_population).astype(jnp.float32)
    position = offset + lax.iota(jnp.int32, local_cells)
    batch_of = jnp.sum((batch_ends[:, None] <= position[None, :]).astype(jnp.int32), axis=0)
    first_batch = batch_of[0]
    last_batch = batch_of[local_cells - 1]
    group_affinity = observation_affinity(latent_coordinates, group_means, entropy_scaling)
    expected_occupancy = probabilistic_responsibility(group_affinity)

    def count_step(batch_id, running):
        in_batch = (batch_of == batch_id).astype(jnp.float32)
        single_observation = jnp.dot(
            expected_occupancy, in_batch, precision=highest, preferred_element_type=jnp.float32
        )
        return lax.dynamic_update_slice(
            running, single_observation[:, None], (jnp.int32(0), batch_id)
        )

    counts = lax.fori_loop(
        first_batch, last_batch + 1, count_step, jnp.zeros((clusters, batches), jnp.float32)
    )
    counts = lax.psum(counts, ("cells", "grp"))
    totals = jnp.sum(counts, axis=1)
    expected = sample_population.astype(jnp.float32)[None, :] * totals[:, None] / cells_total
    penalty = diversity * jnp.log((counts + 1.0) / (expected + 1.0))

    def penalty_step(batch_id, running):
        in_batch = (batch_of == batch_id).astype(jnp.float32)
        column = lax.dynamic_index_in_dim(penalty, batch_id, 1, keepdims=True)
        return running + column * in_batch[None, :]

    cell_penalty = lax.fori_loop(
        first_batch, last_batch + 1, penalty_step, jnp.zeros((clusters, local_cells), jnp.float32)
    )
    assign = probabilistic_responsibility(group_affinity - cell_penalty)
    augmented = jnp.concatenate(
        [jnp.ones((1, local_cells), jnp.float32), latent_coordinates], axis=0
    )

    def moment_step(batch_id, running):
        in_batch = (batch_of == batch_id).astype(jnp.float32)
        contiguous_portion = jnp.einsum(
            "kn,dn->kd", assign * in_batch[None, :], augmented, precision=highest
        )
        return lax.dynamic_update_slice(
            running, contiguous_portion[:, :, None], (jnp.int32(0), jnp.int32(0), batch_id)
        )

    moments = lax.fori_loop(
        first_batch,
        last_batch + 1,
        moment_step,
        jnp.zeros((clusters, num_pcs + 1, batches), jnp.float32),
    )
    devices_flat = lax.axis_size("cells") * lax.axis_size("grp")
    most_cells = 2 * local_cells * devices_flat // batches
    reach = (most_cells - 2) // local_cells + 1
    begins_here = (batch_starts >= offset) & (batch_starts < offset + local_cells)
    owner_mask = begins_here.astype(jnp.float32)
    head_owned = begins_here[first_batch]
    head_column = lax.dynamic_index_in_dim(moments, first_batch, 2, keepdims=False)
    sent_stats = jnp.where(head_owned, 0.0, 1.0) * head_column
    sent_tag = jnp.where(head_owned, 0.0, first_batch.astype(jnp.float32) + 1.0) * jnp.ones(
        (1,), jnp.float32
    )
    completed = moments
    for hop in range(1, reach + 1):
        got_stats, got_tag = from_behind((sent_stats, sent_tag), ("cells", "grp"), -hop)
        got_id = jnp.maximum(got_tag[0].astype(jnp.int32) - 1, 0)
        accept = jnp.where((got_tag[0] > 0.5) & begins_here[got_id], 1.0, 0.0)
        single_observation = (
            lax.dynamic_index_in_dim(completed, got_id, 2, keepdims=False) + accept * got_stats
        )
        completed = lax.dynamic_update_slice(
            completed, single_observation[:, :, None], (jnp.int32(0), jnp.int32(0), got_id)
        )
    completed = completed * owner_mask[None, None, :]
    weight, right_side, mass_total, moment_total = lax.psum(
        batch_parts(completed, sample_shrinkage_lambda), ("cells", "grp")
    )
    coefficients = slopes_of(completed, sample_shrinkage_lambda, weight, right_side)
    every_centroid = moment_total / (1.0 + mass_total)[:, None]
    new_centroids = lax.dynamic_slice_in_dim(
        every_centroid, lax.axis_index("cells") * owned, owned, 0
    )
    tail_owned = begins_here[last_batch]
    tail_column = lax.dynamic_index_in_dim(coefficients, last_batch, 2, keepdims=False)
    tail_send = jnp.where(tail_owned, 1.0, 0.0) * tail_column
    tail_tag = jnp.where(tail_owned, last_batch.astype(jnp.float32) + 1.0, 0.0) * jnp.ones(
        (1,), jnp.float32
    )
    head_fix = jnp.zeros_like(tail_column)
    for hop in range(1, reach + 1):
        got_coef, got_tag = from_behind((tail_send, tail_tag), ("cells", "grp"), hop)
        match = got_tag[0] == first_batch.astype(jnp.float32) + 1.0
        head_fix = jnp.where(match, got_coef, head_fix)
    own_head = lax.dynamic_index_in_dim(coefficients, first_batch, 2, keepdims=False)
    head_final = jnp.where(head_owned, own_head, head_fix)
    coefficients = lax.dynamic_update_slice(
        coefficients, head_final[:, :, None], (jnp.int32(0), jnp.int32(0), first_batch)
    )

    def correct_step(batch_id, running):
        in_batch = (batch_of == batch_id).astype(jnp.float32)
        slope_table = lax.dynamic_index_in_dim(coefficients, batch_id, 2, keepdims=False)
        moved = jnp.einsum("kd,kn->dn", slope_table, assign * in_batch[None, :], precision=highest)
        return running - moved

    corrected = lax.fori_loop(first_batch, last_batch + 1, correct_step, latent_coordinates)
    return (corrected, new_centroids)


SLOTS = 16
MESH = pl.DeviceIdType.MESH
f32 = jnp.float32
bf16 = jnp.bfloat16


def hi_lo(value):
    hi = value.astype(bf16)
    return hi, (value - hi.astype(f32)).astype(bf16)


def nt_dot(a, b):
    return lax.dot_general(a, b, (((1,), (1,)), ((), ())), preferred_element_type=f32)


def nn_dot(a, b):
    return jnp.dot(a, b, preferred_element_type=f32)


def iota(shape, axis):
    return lax.broadcasted_iota(jnp.int32, shape, axis)


def fiota(shape, axis):
    return iota(shape, axis).astype(f32)


def fused_kernel(
    cells_size, grp_size, chunk,
    x_ref, means_ref, entropy_ref, ridge_ref, population_ref,
    out_ref, centroid_ref,
    xs, xt, scores, mask, spread, zh, zl, send1, recv1, send_a, recv_a, slab1, slab2, slab3,
    sem1, sem_a, sem_b, sem_c, sem_d,
):
    num_pcs, local = x_ref.shape
    clusters = means_ref.shape[0]
    batches = population_ref.shape[1]
    owned = centroid_ref.shape[0]
    rows = SLOTS * clusters
    wide = xs.shape[0]
    devices = cells_size * grp_size
    chunks = local // chunk
    cell_index = lax.axis_index("cells")
    grp_index = lax.axis_index("grp")
    me = cell_index * grp_size + grp_index

    def at(flat):
        return {"cells": flat // grp_size, "grp": lax.rem(flat, grp_size)}

    barrier = pltpu.get_barrier_semaphore()
    for step in range(1, devices):
        pl.semaphore_signal(
            barrier, inc=1, device_id=at(lax.rem(me + step, devices)), device_id_type=MESH
        )

    population = population_ref[...].astype(f32)
    ridge = ridge_ref[...]
    offset = (me * local).astype(f32)
    ends = jnp.sum(
        jnp.where(iota((batches, batches), 1) <= iota((batches, batches), 0), population, 0.0),
        axis=1, keepdims=True,
    )

    def batch_at(position):
        return jnp.sum(jnp.where(ends <= position, 1.0, 0.0), axis=0, keepdims=True)

    first = batch_at(offset)
    last = batch_at(offset + (local - 1.0))
    prev_last = batch_at(offset - 1.0)
    next_first = batch_at(offset + float(local))
    tail_slot = last - first
    from_prev = jnp.where((prev_last == first) & (first * 0.0 + offset > 0.0), 1.0, 0.0)
    from_next = jnp.where(next_first == last, 1.0, 0.0)
    lane = fiota((SLOTS, batches), 1)
    slot = first + fiota((SLOTS, 1), 0)
    slot_start = jnp.sum(jnp.where(lane < slot, population, 0.0), axis=1, keepdims=True)
    slot_size = jnp.sum(jnp.where(lane == slot, population, 0.0), axis=1, keepdims=True)
    slot_end = slot_start + slot_size
    cells_total = jnp.sum(population, axis=1, keepdims=True)
    size_row = jnp.sum(
        jnp.where(iota((SLOTS, SLOTS), 0) == iota((SLOTS, SLOTS), 1), slot_size, 0.0),
        axis=0, keepdims=True,
    )
    row_slot = first + (iota((rows, 1), 0) // clusters).astype(f32)
    row_ridge = jnp.sum(
        jnp.where(fiota((rows, batches), 1) == row_slot, ridge, 0.0), axis=1, keepdims=True
    )
    row_ridge = jnp.where(row_slot < float(batches), row_ridge, 1.0)

    means = means_ref[...]
    lengths = jnp.sum(means * means, axis=1, keepdims=True)
    twice = 2.0 * entropy_ref[...]

    xs[num_pcs - num_pcs % 8 :, :] = jnp.where(
        iota((wide - num_pcs + num_pcs % 8, local), 0) == num_pcs % 8, 1.0, 0.0
    )
    xs[:num_pcs, :] = x_ref[...]

    def scores_step(index, counts):
        at_lanes = pl.ds(pl.multiple_of(index * chunk, chunk), chunk)
        block = xs[:, at_lanes]
        dots = jnp.dot(
            means, block[:num_pcs], precision=highest, preferred_element_type=f32
        )
        affinity = (2.0 * dots - lengths) / twice
        scores[:, at_lanes] = affinity
        prior = probabilistic_responsibility(affinity)
        position = offset + (index * chunk).astype(f32) + fiota((1, chunk), 1)
        inside = jnp.where(
            (position >= slot_start) & (position < slot_end), 1.0, 0.0
        ).astype(bf16)
        mask[:, at_lanes] = inside
        prior_hi, prior_lo = hi_lo(prior)
        return counts + nt_dot(prior_hi, inside) + nt_dot(prior_lo, inside)

    counts = lax.fori_loop(0, chunks, scores_step, jnp.zeros((clusters, SLOTS), f32))

    slot_lane = fiota((clusters, SLOTS), 1)
    total = jnp.sum(counts, axis=1, keepdims=True)
    tail = jnp.sum(jnp.where(slot_lane == tail_slot, counts, 0.0), axis=1, keepdims=True)
    width = send1.shape[2]
    row_lane = iota((clusters, width), 1)
    row_k = iota((clusters, width), 0)
    packed = (
        jnp.where(row_lane == row_k, total, 0.0)
        + jnp.where(row_lane == row_k + clusters, counts[:, :1], 0.0)
        + jnp.where(row_lane == row_k + 2 * clusters, tail, 0.0)
    )
    packed = jnp.sum(packed, axis=0, keepdims=True)
    send1[0] = packed
    pl.semaphore_wait(barrier, devices - 1)
    for step in range(1, devices):
        pltpu.make_async_remote_copy(
            src_ref=send1.at[0], dst_ref=recv1.at[step - 1],
            send_sem=sem1.at[0], recv_sem=sem1.at[1],
            device_id=at(lax.rem(me + step, devices)), device_id_type=MESH,
        ).start()

    def ready_step(index, unused):
        at_lanes = pl.ds(pl.multiple_of(index * chunk, chunk), chunk)
        hi, lo = hi_lo(xs[:, at_lanes].T)
        xt[at_lanes, :] = jnp.concatenate([hi, lo], axis=1)
        inside = mask[:, at_lanes]
        for j in range(SLOTS):
            spread[j * clusters : (j + 1) * clusters, at_lanes] = jnp.broadcast_to(
                inside[j : j + 1, :], (clusters, chunk)
            )
        return unused

    lax.fori_loop(0, chunks, ready_step, 0)
    pltpu.make_async_copy(recv1, recv1, sem1.at[1]).wait()

    def column(row, part):
        return jnp.sum(
            jnp.where(row_lane == row_k + part * clusters, row, 0.0), axis=1, keepdims=True
        )

    everyone = packed
    for step in range(1, devices):
        everyone = everyone + recv1[step - 1]
    totals = column(everyone, 0)
    head_more = from_prev * column(recv1[0], 2)
    tail_more = from_next * column(recv1[devices - 2], 1)
    counts = (
        counts
        + jnp.where(slot_lane == 0.0, head_more, 0.0)
        + jnp.where(slot_lane == tail_slot, tail_more, 0.0)
    )
    expected = size_row * totals / cells_total
    penalty = diversity * jnp.log((counts + 1.0) / (expected + 1.0))
    pen_hi = penalty.astype(bf16)
    rest = penalty - pen_hi.astype(f32)
    pen_mid, pen_lo = hi_lo(rest)
    pen_cat = jnp.concatenate([pen_hi, pen_mid, pen_lo], axis=0)

    def assign_step(index, moments):
        at_lanes = pl.ds(pl.multiple_of(index * chunk, chunk), chunk)
        inside = mask[:, at_lanes]
        cell_penalty = nn_dot(pen_cat, inside)
        cell_penalty = (
            cell_penalty[:clusters]
            + cell_penalty[clusters : 2 * clusters]
            + cell_penalty[2 * clusters :]
        )
        assign = probabilistic_responsibility(scores[:, at_lanes] - cell_penalty)
        hi, lo = hi_lo(assign)
        for j in range(SLOTS):
            here = spread[j * clusters : (j + 1) * clusters, at_lanes]
            zh[j * clusters : (j + 1) * clusters, at_lanes] = hi * here
            zl[j * clusters : (j + 1) * clusters, at_lanes] = lo * here
        cells = xt[at_lanes, :]
        return moments + nn_dot(zh[:, at_lanes], cells) + nn_dot(zl[:, at_lanes], cells)

    moments = lax.fori_loop(0, chunks, assign_step, jnp.zeros((rows, 2 * wide), f32))
    moments = moments[:, :wide] + moments[:, wide:]

    def of_slot(array, j):
        return array[j * clusters : (j + 1) * clusters]

    tail_block = jnp.zeros((clusters, wide), f32)
    for j in range(SLOTS):
        tail_block = tail_block + jnp.where(tail_slot == float(j), of_slot(moments, j), 0.0)
    send_a[0] = tail_block
    send_a[1] = of_slot(moments, 0)
    to_next = pltpu.make_async_remote_copy(
        src_ref=send_a.at[0], dst_ref=recv_a.at[0], send_sem=sem_a.at[0], recv_sem=sem_a.at[1],
        device_id=at(lax.rem(me + 1, devices)), device_id_type=MESH,
    )
    to_prev = pltpu.make_async_remote_copy(
        src_ref=send_a.at[1], dst_ref=recv_a.at[1], send_sem=sem_a.at[2], recv_sem=sem_a.at[3],
        device_id=at(lax.rem(me + devices - 1, devices)), device_id_type=MESH,
    )
    to_next.start()
    to_prev.start()
    to_next.wait_recv()
    to_prev.wait_recv()
    head_more = from_prev * recv_a[0]
    tail_more = from_next * recv_a[1]
    full = []
    for j in range(SLOTS):
        block = of_slot(moments, j) + jnp.where(tail_slot == float(j), tail_more, 0.0)
        full.append(block + head_more if j == 0 else block)

    shrunk_sum = jnp.zeros((clusters, wide), f32)
    plain_sum = jnp.zeros((clusters, wide), f32)
    for j in range(SLOTS):
        lam = of_slot(row_ridge, j)
        shrink = lam / (full[j][:, num_pcs : num_pcs + 1] + lam)
        shrunk_sum = shrunk_sum + shrink * of_slot(moments, j)
        plain_sum = plain_sum + of_slot(moments, j)

    def send(slab, value, axis, index, size, sem):
        slab[index] = value
        copies = []
        for step in range(1, size):
            copies.append(
                pltpu.make_async_remote_copy(
                    src_ref=slab.at[index], dst_ref=slab.at[index],
                    send_sem=sem.at[0, step], recv_sem=sem.at[1, step],
                    device_id={axis: lax.rem(index + step, size)}, device_id_type=MESH,
                )
            )
        for copy in copies:
            copy.start()
        return copies

    def gathered(slab, size, copies):
        for copy in copies:
            copy.wait_recv()
        result = slab[0]
        for step in range(1, size):
            result = result + slab[step]
        return result

    part = jnp.concatenate([shrunk_sum, plain_sum], axis=1)
    copies_b = send(slab1, part, "grp", grp_index, grp_size, sem_b)
    part = gathered(slab1, grp_size, copies_b)
    copies_c = send(slab2, part[:, :wide], "cells", cell_index, cells_size, sem_c)
    copies_d = send(slab3, part[:, wide:], "cells", cell_index, cells_size, sem_d)
    shrunk_sum = gathered(slab2, cells_size, copies_c)
    intercept = shrunk_sum / (intercept_ridge + shrunk_sum[:, num_pcs : num_pcs + 1])

    slopes = []
    for j in range(SLOTS):
        mass = full[j][:, num_pcs : num_pcs + 1]
        slopes.append((full[j] - mass * intercept) / (mass + of_slot(row_ridge, j)))
    slopes = jnp.concatenate(slopes, axis=0).T
    slope_hi, slope_lo = hi_lo(slopes)
    slope_cat = jnp.concatenate([slope_hi, slope_lo], axis=0)

    def correct_step(index, unused):
        at_lanes = pl.ds(pl.multiple_of(index * chunk, chunk), chunk)
        first_part = nn_dot(slope_cat, zh[:, at_lanes])
        second_part = nn_dot(slope_hi, zl[:, at_lanes])
        moved = first_part[:wide] + first_part[wide:] + second_part
        out_ref[:, at_lanes] = (xs[:, at_lanes] - moved)[:num_pcs]
        return unused

    lax.fori_loop(0, chunks, correct_step, 0)

    plain_sum = gathered(slab3, cells_size, copies_d)
    centroids = plain_sum / (1.0 + plain_sum[:, num_pcs : num_pcs + 1])
    for r in range(owned):
        picked = jnp.where(
            iota((clusters, wide), 0) == cell_index * owned + r, centroids, 0.0
        )
        centroid_ref[r : r + 1, :] = jnp.sum(picked, axis=0, keepdims=True)[:, :num_pcs]

    pltpu.make_async_copy(recv1, recv1, sem1.at[0]).wait()
    to_next.wait_send()
    to_prev.wait_send()
    for copy in copies_b + copies_c + copies_d:
        copy.wait_send()


def fused(latent_coordinates, group_means, entropy_scaling, ridge, population):
    num_pcs, local = latent_coordinates.shape
    clusters = group_means.shape[0]
    cells_size, grp_size = lax.axis_size("cells"), lax.axis_size("grp")
    devices = cells_size * grp_size
    rows = SLOTS * clusters
    wide = -(-(num_pcs + 1) // 64) * 64
    width = -(-3 * clusters // 128) * 128
    vmem = pl.BlockSpec(memory_space=pltpu.VMEM)
    dma = pltpu.SemaphoreType.DMA
    return pl.pallas_call(
        functools.partial(fused_kernel, cells_size, grp_size, min(local, 2048)),
        out_shape=(
            jax.ShapeDtypeStruct((num_pcs, local), f32),
            jax.ShapeDtypeStruct((clusters // cells_size, num_pcs), f32),
        ),
        in_specs=[vmem] * 5,
        out_specs=(vmem, vmem),
        scratch_shapes=[
            pltpu.VMEM((wide, local), f32),
            pltpu.VMEM((local, 2 * wide), bf16),
            pltpu.VMEM((clusters, local), f32),
            pltpu.VMEM((SLOTS, local), bf16),
            pltpu.VMEM((rows, local), bf16),
            pltpu.VMEM((rows, local), bf16),
            pltpu.VMEM((rows, local), bf16),
            pltpu.VMEM((1, 1, width), f32),
            pltpu.VMEM((devices - 1, 1, width), f32),
            pltpu.VMEM((2, clusters, wide), f32),
            pltpu.VMEM((2, clusters, wide), f32),
            pltpu.VMEM((grp_size, clusters, 2 * wide), f32),
            pltpu.VMEM((cells_size, clusters, wide), f32),
            pltpu.VMEM((cells_size, clusters, wide), f32),
            dma((2,)),
            dma((4,)),
            dma((2, grp_size)),
            dma((2, cells_size)),
            dma((2, cells_size)),
        ],
        compiler_params=pltpu.CompilerParams(
            collective_id=0, has_side_effects=True, vmem_limit_bytes=40 * 2**20
        ),
    )(
        latent_coordinates, group_means, entropy_scaling[:, None], ridge[None, :],
        population[None, :],
    )


def step(
    latent_coordinates, group_means, entropy_scaling, sample_shrinkage_lambda, sample_population
):
    local = latent_coordinates.shape[1]
    batches = sample_population.shape[0]
    devices = lax.axis_size("cells") * lax.axis_size("grp")
    args = (
        latent_coordinates, group_means, entropy_scaling, sample_shrinkage_lambda,
        sample_population,
    )
    if 2 * local * devices // batches > local:
        return body(*args)
    ends = jnp.cumsum(sample_population)
    crowded = jnp.any(
        ends[SLOTS - 1 : batches - 1] // local == (ends[: batches - SLOTS] - 1) // local
    )
    return lax.cond(crowded, body, fused, *args)


def solution(mesh):
    return jax.shard_map(
        step,
        mesh=mesh,
        in_specs=(P(None, ("cells", "grp")), P(), P(), P(), P()),
        out_specs=(P(None, ("cells", "grp")), P("cells", None)),
        check_vma=False,
    )
```
